32 devices in a mesh: px: 2 (over x), py: 16 (over z, y, core).
Axes of the slice: x: 2, y: 2, z: 4, core: 2. Of those that a mesh axis runs over, the one named last changes fastest.
Arguments:
- populations: float32 [19, 2, 256, 512], P(None, None, ('py', 'px')), may hold values from 0.02 to 0.12
- pore: int32 [2, 256, 512], P(None, ('py', 'px')), may hold values 0 or 1
Outputs:
- flow: float32 [19, 2, 256, 512], P(None, None, 'py', 'px')
The draws below stay inside these ranges and needn't reach their ends.
All inputs are finite; a program needn't handle non-finite values. No bound on the sum of `pore` on one device may be relied on, other than what follows from the above.
Results may differ from the reference program's by a relative error of at most 0.0001.
Values sent between devices are 32-bit elements; how exact they have to be, the bound alone decides.
A program may use at most 128 MiB of HBM per device.

```python
import jax
import jax.numpy as jnp

Q = 19
NZ = 2
STEPS = 2
NX = 512
NY = 256


def with_ends(values, key, least, largest):
    extent = values.shape
    index_at = [jax.random.randint(jax.random.fold_in(key, axis), (), 0, extent[axis]) for axis in range(len(extent))]
    values = values.at[tuple(index_at)].set(least)
    longest = extent.index(max(extent))
    index_at[longest] = (index_at[longest] + 1) % extent[longest]
    return values.at[tuple(index_at)].set(largest)


def block_levels(rng, dims, shards, low, top_value):
    factor_of = 1.0
    for dim, blocks in shards:
        heights = jax.random.uniform(jax.random.fold_in(jax.random.fold_in(rng, 6), dim), (blocks,), jnp.float32, low / len(shards), top_value / len(shards))
        factor_of = factor_of * jnp.repeat(jnp.exp(heights), dims[dim] // blocks).reshape((-1,) + (1,) * (len(dims) - 1 - dim))
    return factor_of


def setup_inputs(seed: int = 0) -> dict:
    streams_of = jax.random.split(jax.random.key(seed), 3)
    populations = jnp.clip(0.02 + 0.09999999776482582 * jax.random.uniform(streams_of[0], (Q, NZ, NY, NX), jnp.float32) ** block_levels(streams_of[0], (Q, NZ, NY, NX), ((2, 32),), -0.2, 0.2), 0.02, 0.12)
    pore = with_ends((jax.random.randint(streams_of[1], (NZ, NY, NX), 0, 4) < 3).astype(jnp.int32), jax.random.fold_in(streams_of[1], 1), 0, 1)
    return {"populations": populations, "pore": pore}


lattice_velocity = [(0, 0, 0), (1, 0, 0), (-1, 0, 0), (0, 1, 0), (0, -1, 0), (0, 0, 1), (0, 0, -1),
                    (1, 1, 0), (-1, -1, 0), (1, -1, 0), (-1, 1, 0), (1, 0, 1), (-1, 0, -1), (1, 0, -1),
                    (-1, 0, 1), (0, 1, 1), (0, -1, -1), (0, 1, -1), (0, -1, 1)]
lattice_weights = [1.0 / 3.0] + [1.0 / 18.0] * 6 + [1.0 / 36.0] * 12
opposite = [0, 2, 1, 4, 3, 6, 5, 8, 7, 10, 9, 12, 11, 14, 13, 16, 15, 18, 17]
relax_time = 0.8
body_force = 0.005


def moment(fields, column):
    total = jnp.zeros_like(fields[0])
    for slot in range(len(lattice_velocity)):
        vector = lattice_velocity[slot]
        if vector[column] != 0:
            total = total + float(vector[column]) * fields[slot]
    return total


def collide(fields, fluid):
    density = jnp.where(fluid > 0.5, jnp.sum(fields, axis=0), 1.0)
    vel_first = moment(fields, 0) / density
    vel_second = moment(fields, 1) / density
    vel_third = moment(fields, 2) / density + relax_time * body_force
    speed = vel_first * vel_first + vel_second * vel_second + vel_third * vel_third
    result = []
    for slot in range(len(lattice_velocity)):
        vector = lattice_velocity[slot]
        along = vector[0] * vel_first + vector[1] * vel_second + vector[2] * vel_third
        equil = lattice_weights[slot] * density * (1.0 + 3.0 * along + 4.5 * along * along - 1.5 * speed)
        result.append(fields[slot] - (fields[slot] - equil) / relax_time)
    return jnp.stack(result) * fluid[None]


def reference(populations, pore):
    fluid = pore.astype(jnp.float32)
    fields = populations
    for step in range(STEPS):
        post = collide(fields, fluid)
        result = []
        for slot in range(len(lattice_velocity)):
            vector = lattice_velocity[slot]
            source = jnp.roll(post[slot], (vector[2], vector[1], vector[0]), axis=(0, 1, 2))
            open_cell = jnp.roll(fluid, (vector[2], vector[1], vector[0]), axis=(0, 1, 2))
            result.append(jnp.where(open_cell > 0.5, source, post[opposite[slot]]))
        fields = jnp.stack(result) * fluid[None]
    return fields
```

```python
import functools

import jax
import jax.numpy as jnp
from jax import lax
from jax.experimental import pallas as pl
from jax.experimental.pallas import tpu as pltpu
from jax.sharding import PartitionSpec as P

STEPS = 2
MESH = pl.DeviceIdType.MESH

lattice_velocity = [
    (0, 0, 0),
    (1, 0, 0),
    (-1, 0, 0),
    (0, 1, 0),
    (0, -1, 0),
    (0, 0, 1),
    (0, 0, -1),
    (1, 1, 0),
    (-1, -1, 0),
    (1, -1, 0),
    (-1, 1, 0),
    (1, 0, 1),
    (-1, 0, -1),
    (1, 0, -1),
    (-1, 0, 1),
    (0, 1, 1),
    (0, -1, -1),
    (0, 1, -1),
    (0, -1, 1),
]
lattice_weights = [1.0 / 3.0] + [1.0 / 18.0] * 6 + [1.0 / 36.0] * 12
opposite = [0, 2, 1, 4, 3, 6, 5, 8, 7, 10, 9, 12, 11, 14, 13, 16, 15, 18, 17]
relax_time = 0.8
body_force = 0.005

Q = len(lattice_velocity)
LANES = 128
ROWS = 8
HALO = 2
SOLID = -3.0e38


def collide_tile(fields, fluid):
    keep = 1.0 - 1.0 / relax_time
    gain = 1.0 / relax_time
    is_open = fluid > 0.5
    density = functools.reduce(lambda x, y: x + y, fields)
    density = jnp.where(is_open, density, 1.0)
    inverse = 1.0 / density
    vel = []
    for column in range(3):
        plus = [fields[s] for s in range(Q) if lattice_velocity[s][column] > 0]
        minus = [fields[s] for s in range(Q) if lattice_velocity[s][column] < 0]
        total = functools.reduce(lambda x, y: x + y, plus) - functools.reduce(lambda x, y: x + y, minus)
        vel.append(total * inverse)
    vel[2] = vel[2] + relax_time * body_force
    speed = vel[0] * vel[0] + vel[1] * vel[1] + vel[2] * vel[2]
    base = 1.0 - 1.5 * speed
    result = [None] * Q
    scaled = {w: density * (gain * w) for w in sorted(set(lattice_weights))}
    result[0] = jnp.where(is_open, keep * fields[0] + scaled[lattice_weights[0]] * base, SOLID)
    for slot in range(1, Q, 2):
        other = opposite[slot]
        along = None
        for column in range(3):
            sign = lattice_velocity[slot][column]
            if sign == 0:
                continue
            term = vel[column]
            if along is None:
                along = term if sign > 0 else -term
            else:
                along = along + term if sign > 0 else along - term
        weight = scaled[lattice_weights[slot]]
        triple = 3.0 * along
        even = weight * (base + 0.5 * triple * triple)
        odd = weight * triple
        result[slot] = jnp.where(is_open, keep * fields[slot] + (even + odd), SOLID)
        result[other] = jnp.where(is_open, keep * fields[other] + (even - odd), SOLID)
    return result


def kernel(
    across, along, pop_ref, pore_ref, out_ref,
    cells, strip, voxels, packs, edges, post,
    local_sem, a_send, a_recv, b_send, b_recv, e_send, e_recv, h_send, h_recv,
):
    _, planes, rows, _ = pop_ref.shape
    height = across * rows
    width = out_ref.shape[3]
    tall = height + ROWS
    wide = width + LANES
    groups = edges.shape[0]
    per_group = LANES // 4
    me = lax.axis_index("px")
    here = lax.axis_index("py")
    up = lax.rem(here + along - 1, along)
    down = lax.rem(here + 1, along)

    own_rows = pl.ds(pl.multiple_of(me * rows, rows), rows)
    own_cols = pl.ds(pl.multiple_of(me * width, width), width)
    load_pore = pltpu.make_async_copy(pore_ref, voxels, local_sem.at[0])
    load_strip = pltpu.make_async_copy(pop_ref, strip.at[0:Q], local_sem.at[1])
    load_own = pltpu.make_async_copy(
        pop_ref.at[:, :, :, own_cols], cells.at[0:Q, :, own_rows, 0:width], local_sem.at[2]
    )
    load_pore.start()
    load_strip.start()
    load_own.start()

    barrier = pltpu.get_barrier_semaphore()
    for step in range(1, across):
        pl.semaphore_signal(barrier, inc=1, device_id=(lax.rem(me + step, across), here), device_id_type=MESH)
    for to in (up, down):
        pl.semaphore_signal(barrier, inc=1, device_id=(me, to), device_id_type=MESH)

    load_pore.wait()
    strip[Q] = voxels[...].astype(jnp.float32)
    cells[Q, :, own_rows, 0:width] = voxels[:, :, own_cols].astype(jnp.float32)
    load_strip.wait()

    lane = lax.broadcasted_iota(jnp.int32, (rows, LANES), 1)
    total = across * width
    for target in range(across):
        first = (target + 1) * width % total
        last = (target * width - LANES) % total
        for group in range(groups):
            packed = jnp.zeros((rows, LANES), jnp.float32)
            for place in range(per_group):
                slab = group * per_group + place
                if slab >= (Q + 1) * planes:
                    break
                field, plane = slab // planes, slab % planes
                edge = jnp.where(
                    lane < LANES // 2,
                    strip[field, plane, :, first : first + LANES],
                    strip[field, plane, :, last : last + LANES],
                )
                if place == 0:
                    packed = edge
                else:
                    moved = pltpu.roll(edge, 4 * place, 1)
                    packed = jnp.where((lane >= 4 * place - 2) & (lane < 4 * place + 2), moved, packed)
            packs[target, group] = packed
    edges[:, own_rows, :] = packs[me]

    pl.semaphore_wait(barrier, across - 1 + 2)

    def near(source):
        return (rows - HALO, rows) if source == across - 1 else (0, HALO)

    def far(source):
        return (0, rows - HALO) if source == across - 1 else (HALO, rows)

    def strip_copy(source, target, part, send, recv):
        low, high = part(source)
        return pltpu.make_async_remote_copy(
            src_ref=strip.at[:, :, low:high, target * width : (target + 1) * width],
            dst_ref=cells.at[:, :, source * rows + low : source * rows + high, 0:width],
            send_sem=send.at[target],
            recv_sem=recv.at[source],
            device_id=(target, here),
            device_id_type=MESH,
        )

    def edge_copy(source, target):
        return pltpu.make_async_remote_copy(
            src_ref=packs.at[target],
            dst_ref=edges.at[:, source * rows : (source + 1) * rows, :],
            send_sem=e_send.at[target],
            recv_sem=e_recv.at[source],
            device_id=(target, here),
            device_id_type=MESH,
        )

    def halo_copies(way):
        if way == 0:
            source, dest, to = 0, height, up
        else:
            source, dest, to = height - HALO, tall - HALO, down
        return [
            pltpu.make_async_remote_copy(
                src_ref=cells.at[:, :, source : source + HALO, 0:width],
                dst_ref=cells.at[:, :, dest : dest + HALO, 0:width],
                send_sem=h_send.at[2 * way],
                recv_sem=h_recv.at[2 * way],
                device_id=(me, to),
                device_id_type=MESH,
            ),
            pltpu.make_async_remote_copy(
                src_ref=edges.at[:, source : source + HALO, :],
                dst_ref=edges.at[:, dest : dest + HALO, :],
                send_sem=h_send.at[2 * way + 1],
                recv_sem=h_recv.at[2 * way + 1],
                device_id=(me, to),
                device_id_type=MESH,
            ),
        ]

    for mine in range(across):

        @pl.when(me == mine)
        def _():
            others = [(mine + step) % across for step in range(1, across)]
            for target in others:
                strip_copy(mine, target, near, a_send, a_recv).start()
                edge_copy(mine, target).start()
            for target in others:
                strip_copy(mine, target, far, b_send, b_recv).start()
            load_own.wait()
            sources = ((0, 0), (across - 1, 1))
            for source, way in sources:
                if source == mine:
                    for copy in halo_copies(way):
                        copy.start()
            for source, way in sources:
                if source != mine:
                    strip_copy(source, mine, near, a_send, a_recv).wait_recv()
                    edge_copy(source, mine).wait_recv()
                    for copy in halo_copies(way):
                        copy.start()
            for source in others:
                if source not in (0, across - 1):
                    strip_copy(source, mine, near, a_send, a_recv).wait_recv()
                    edge_copy(source, mine).wait_recv()
                strip_copy(source, mine, far, b_send, b_recv).wait_recv()
            for target in others:
                strip_copy(mine, target, near, a_send, a_recv).wait_send()
                edge_copy(mine, target).wait_send()
                strip_copy(mine, target, far, b_send, b_recv).wait_send()
            for way in range(2):
                for copy in halo_copies(way):
                    copy.wait()

    tiles = tall // ROWS

    def unpack(tile, carry):
        at = pl.ds(pl.multiple_of(tile * ROWS, ROWS), ROWS)
        for slab in range((Q + 1) * planes):
            group, place = slab // per_group, slab % per_group
            packed = edges[group, at, :]
            moved = pltpu.roll(packed, LANES - 4 * place, 1) if place else packed
            cells[slab // planes, slab % planes, at, width:wide] = moved
        return carry

    lax.fori_loop(0, tiles, unpack, 0)

    def collide(tile, carry):
        at = pl.ds(pl.multiple_of(tile * ROWS, ROWS), ROWS)
        for plane in range(planes):
            for col in range(0, wide, LANES):
                fields = [cells[slot, plane, at, col : col + LANES] for slot in range(Q)]
                result = collide_tile(fields, cells[Q, plane, at, col : col + LANES])
                for slot in range(Q):
                    post[slot, plane, at, col : col + LANES] = result[slot]
        return carry

    for step in range(STEPS):
        lax.fori_loop(0, tiles, collide, 0)
        for plane in range(planes):
            is_open = cells[Q, plane] > 0.5
            for slot in range(Q):
                vector = lattice_velocity[slot]
                value = post[slot, (plane - vector[2]) % planes]
                if vector[1]:
                    value = pltpu.roll(value, vector[1] % tall, 0)
                if vector[0]:
                    value = pltpu.roll(value, vector[0] % wide, 1)
                if slot:
                    value = jnp.where(value != SOLID, value, post[opposite[slot], plane])
                value = jnp.where(is_open, value, 0.0)
                if step < STEPS - 1:
                    cells[slot, plane] = value
                else:
                    out_ref[slot, plane] = value[:height, :width]


def body(across, along, populations, pore):
    count, planes, rows, columns = populations.shape
    height = across * rows
    width = columns // across
    tall = height + ROWS
    wide = width + LANES
    groups = -(-(count + 1) * planes * 4 // LANES)
    return pl.pallas_call(
        functools.partial(kernel, across, along),
        out_shape=jax.ShapeDtypeStruct((count, planes, height, width), jnp.float32),
        in_specs=[pl.BlockSpec(memory_space=pl.ANY)] * 2,
        out_specs=pl.BlockSpec(memory_space=pltpu.VMEM),
        scratch_shapes=[
            pltpu.VMEM((count + 1, planes, tall, wide), jnp.float32),
            pltpu.VMEM((count + 1, planes, rows, columns), jnp.float32),
            pltpu.VMEM((planes, rows, columns), jnp.int32),
            pltpu.VMEM((across, groups, rows, LANES), jnp.float32),
            pltpu.VMEM((groups, tall, LANES), jnp.float32),
            pltpu.VMEM((count, planes, tall, wide), jnp.float32),
            pltpu.SemaphoreType.DMA((3,)),
            pltpu.SemaphoreType.DMA((across,)),
            pltpu.SemaphoreType.DMA((across,)),
            pltpu.SemaphoreType.DMA((across,)),
            pltpu.SemaphoreType.DMA((across,)),
            pltpu.SemaphoreType.DMA((across,)),
            pltpu.SemaphoreType.DMA((across,)),
            pltpu.SemaphoreType.DMA((4,)),
            pltpu.SemaphoreType.DMA((4,)),
        ],
        compiler_params=pltpu.CompilerParams(collective_id=0, has_side_effects=True),
    )(populations, pore)


def solution(mesh):
    return jax.shard_map(
        functools.partial(body, mesh.shape["px"], mesh.shape["py"]),
        mesh=mesh,
        in_specs=(P(None, None, ("py", "px"), None), P(None, ("py", "px"), None)),
        out_specs=P(None, None, "py", "px"),
        check_vma=False,
    )
```

```python
import functools

import jax
import jax.numpy as jnp
from jax import lax
from jax.experimental import pallas as pl
from jax.experimental.pallas import tpu as pltpu
from jax.sharding import PartitionSpec as P

STEPS = 2
MESH = pl.DeviceIdType.MESH

lattice_velocity = [
    (0, 0, 0),
    (1, 0, 0),
    (-1, 0, 0),
    (0, 1, 0),
    (0, -1, 0),
    (0, 0, 1),
    (0, 0, -1),
    (1, 1, 0),
    (-1, -1, 0),
    (1, -1, 0),
    (-1, 1, 0),
    (1, 0, 1),
    (-1, 0, -1),
    (1, 0, -1),
    (-1, 0, 1),
    (0, 1, 1),
    (0, -1, -1),
    (0, 1, -1),
    (0, -1, 1),
]
lattice_weights = [1.0 / 3.0] + [1.0 / 18.0] * 6 + [1.0 / 36.0] * 12
opposite = [0, 2, 1, 4, 3, 6, 5, 8, 7, 10, 9, 12, 11, 14, 13, 16, 15, 18, 17]
relax_time = 0.8
body_force = 0.005

Q = len(lattice_velocity)
LANES = 128
ROWS = 8
HALO = 2
VMEM_LIMIT = 24 * 1024 * 1024
SOLID = -3.0e38


def collide_tile(fields, fluid):
    keep = 1.0 - 1.0 / relax_time
    gain = 1.0 / relax_time
    is_open = fluid > 0.5
    density = functools.reduce(lambda x, y: x + y, fields)
    density = jnp.where(is_open, density, 1.0)
    inverse = 1.0 / density
    vel = []
    for column in range(3):
        plus = [fields[s] for s in range(Q) if lattice_velocity[s][column] > 0]
        minus = [fields[s] for s in range(Q) if lattice_velocity[s][column] < 0]
        total = functools.reduce(lambda x, y: x + y, plus) - functools.reduce(lambda x, y: x + y, minus)
        vel.append(total * inverse)
    vel[2] = vel[2] + relax_time * body_force
    speed = vel[0] * vel[0] + vel[1] * vel[1] + vel[2] * vel[2]
    base = 1.0 - 1.5 * speed
    result = [None] * Q
    scaled = {w: density * (gain * w) for w in sorted(set(lattice_weights))}
    result[0] = jnp.where(is_open, keep * fields[0] + scaled[lattice_weights[0]] * base, SOLID)
    for slot in range(1, Q, 2):
        other = opposite[slot]
        along = None
        for column in range(3):
            sign = lattice_velocity[slot][column]
            if sign == 0:
                continue
            term = vel[column]
            if along is None:
                along = term if sign > 0 else -term
            else:
                along = along + term if sign > 0 else along - term
        weight = scaled[lattice_weights[slot]]
        triple = 3.0 * along
        even = weight * (base + 0.5 * triple * triple)
        odd = weight * triple
        result[slot] = jnp.where(is_open, keep * fields[slot] + (even + odd), SOLID)
        result[other] = jnp.where(is_open, keep * fields[other] + (even - odd), SOLID)
    return result


def kernel(
    across, along, pop_ref, pore_ref, post, mask,
    cells, strip, voxels, packs, edges,
    local_sem, a_send, a_recv, b_send, b_recv, e_send, e_recv, h_send, h_recv,
):
    _, planes, rows, _ = pop_ref.shape
    height = across * rows
    width = pop_ref.shape[3] // across
    tall = height + ROWS
    wide = width + LANES
    groups = edges.shape[0]
    per_group = LANES // 4
    me = lax.axis_index("px")
    here = lax.axis_index("py")
    up = lax.rem(here + along - 1, along)
    down = lax.rem(here + 1, along)

    own_rows = pl.ds(pl.multiple_of(me * rows, rows), rows)
    own_cols = pl.ds(pl.multiple_of(me * width, width), width)
    load_pore = pltpu.make_async_copy(pore_ref, voxels, local_sem.at[0])
    load_strip = pltpu.make_async_copy(pop_ref, strip.at[0:Q], local_sem.at[1])
    load_own = pltpu.make_async_copy(
        pop_ref.at[:, :, :, own_cols], cells.at[0:Q, :, own_rows, 0:width], local_sem.at[2]
    )
    load_pore.start()
    load_strip.start()
    load_own.start()

    barrier = pltpu.get_barrier_semaphore()
    for step in range(1, across):
        pl.semaphore_signal(barrier, inc=1, device_id=(lax.rem(me + step, across), here), device_id_type=MESH)
    for to in (up, down):
        pl.semaphore_signal(barrier, inc=1, device_id=(me, to), device_id_type=MESH)

    load_pore.wait()
    strip[Q] = voxels[...].astype(jnp.float32)
    cells[Q, :, own_rows, 0:width] = voxels[:, :, own_cols].astype(jnp.float32)
    load_strip.wait()

    lane = lax.broadcasted_iota(jnp.int32, (rows, LANES), 1)
    total = across * width
    for target in range(across):
        first = (target + 1) * width % total
        last = (target * width - LANES) % total
        for group in range(groups):
            packed = jnp.zeros((rows, LANES), jnp.float32)
            for place in range(per_group):
                slab = group * per_group + place
                if slab >= (Q + 1) * planes:
                    break
                field, plane = slab // planes, slab % planes
                edge = jnp.where(
                    lane < LANES // 2,
                    strip[field, plane, :, first : first + LANES],
                    strip[field, plane, :, last : last + LANES],
                )
                if place == 0:
                    packed = edge
                else:
                    moved = pltpu.roll(edge, 4 * place, 1)
                    packed = jnp.where((lane >= 4 * place - 2) & (lane < 4 * place + 2), moved, packed)
            packs[target, group] = packed
    edges[:, own_rows, :] = packs[me]

    pl.semaphore_wait(barrier, across - 1 + 2)

    def near(source):
        return (rows - HALO, rows) if source == across - 1 else (0, HALO)

    def far(source):
        return (0, rows - HALO) if source == across - 1 else (HALO, rows)

    def strip_copy(source, target, part, send, recv):
        low, high = part(source)
        return pltpu.make_async_remote_copy(
            src_ref=strip.at[:, :, low:high, target * width : (target + 1) * width],
            dst_ref=cells.at[:, :, source * rows + low : source * rows + high, 0:width],
            send_sem=send.at[target],
            recv_sem=recv.at[source],
            device_id=(target, here),
            device_id_type=MESH,
        )

    def edge_copy(source, target):
        return pltpu.make_async_remote_copy(
            src_ref=packs.at[target],
            dst_ref=edges.at[:, source * rows : (source + 1) * rows, :],
            send_sem=e_send.at[target],
            recv_sem=e_recv.at[source],
            device_id=(target, here),
            device_id_type=MESH,
        )

    def halo_copies(way):
        if way == 0:
            source, dest, to = 0, height, up
        else:
            source, dest, to = height - HALO, tall - HALO, down
        return [
            pltpu.make_async_remote_copy(
                src_ref=cells.at[:, :, source : source + HALO, 0:width],
                dst_ref=cells.at[:, :, dest : dest + HALO, 0:width],
                send_sem=h_send.at[2 * way],
                recv_sem=h_recv.at[2 * way],
                device_id=(me, to),
                device_id_type=MESH,
            ),
            pltpu.make_async_remote_copy(
                src_ref=edges.at[:, source : source + HALO, :],
                dst_ref=edges.at[:, dest : dest + HALO, :],
                send_sem=h_send.at[2 * way + 1],
                recv_sem=h_recv.at[2 * way + 1],
                device_id=(me, to),
                device_id_type=MESH,
            ),
        ]

    for mine in range(across):

        @pl.when(me == mine)
        def _():
            others = [(mine + step) % across for step in range(1, across)]
            for target in others:
                strip_copy(mine, target, near, a_send, a_recv).start()
                edge_copy(mine, target).start()
            for target in others:
                strip_copy(mine, target, far, b_send, b_recv).start()
            load_own.wait()
            sources = ((0, 0), (across - 1, 1))
            for source, way in sources:
                if source == mine:
                    for copy in halo_copies(way):
                        copy.start()
            for source, way in sources:
                if source != mine:
                    strip_copy(source, mine, near, a_send, a_recv).wait_recv()
                    edge_copy(source, mine).wait_recv()
                    for copy in halo_copies(way):
                        copy.start()
            for source in others:
                if source not in (0, across - 1):
                    strip_copy(source, mine, near, a_send, a_recv).wait_recv()
                    edge_copy(source, mine).wait_recv()
                strip_copy(source, mine, far, b_send, b_recv).wait_recv()
            for target in others:
                strip_copy(mine, target, near, a_send, a_recv).wait_send()
                edge_copy(mine, target).wait_send()
                strip_copy(mine, target, far, b_send, b_recv).wait_send()
            for way in range(2):
                for copy in halo_copies(way):
                    copy.wait()

    tiles = tall // ROWS

    def unpack(tile, carry):
        at = pl.ds(pl.multiple_of(tile * ROWS, ROWS), ROWS)
        for slab in range((Q + 1) * planes):
            group, place = slab // per_group, slab % per_group
            packed = edges[group, at, :]
            moved = pltpu.roll(packed, LANES - 4 * place, 1) if place else packed
            cells[slab // planes, slab % planes, at, width:wide] = moved
        return carry

    lax.fori_loop(0, tiles, unpack, 0)

    def collide(tile, carry):
        at = pl.ds(pl.multiple_of(tile * ROWS, ROWS), ROWS)
        for plane in range(planes):
            for col in range(0, wide, LANES):
                fields = [cells[slot, plane, at, col : col + LANES] for slot in range(Q)]
                result = collide_tile(fields, cells[Q, plane, at, col : col + LANES])
                for slot in range(Q):
                    post[slot, plane, at, col : col + LANES] = result[slot]
        return carry

    for step in range(STEPS):
        lax.fori_loop(0, tiles, collide, 0)
        if step < STEPS - 1:
            for plane in range(planes):
                is_open = cells[Q, plane] > 0.5
                for slot in range(Q):
                    cells[slot, plane] = streamed(post, is_open, slot, plane)
    mask[...] = cells[Q]


def streamed(post, is_open, slot, plane):
    _, planes, tall, wide = post.shape
    vector = lattice_velocity[slot]
    value = post[slot, (plane - vector[2]) % planes]
    if vector[1]:
        value = pltpu.roll(value, vector[1] % tall, 0)
    if vector[0]:
        value = pltpu.roll(value, vector[0] % wide, 1)
    if slot:
        value = jnp.where(value != SOLID, value, post[opposite[slot], plane])
    return jnp.where(is_open, value, 0.0)


def finish(post, mask, out_ref, flow, sems):
    _, planes, height, width = flow.shape
    copies = []
    for slot in range(Q):
        for plane in range(planes):
            value = streamed(post, mask[plane] > 0.5, slot, plane)
            flow[slot, plane] = value[:height, :width]
        copies.append(pltpu.make_async_copy(flow.at[slot], out_ref.at[slot], sems.at[slot]))
        if slot:
            copies[slot - 1].start()
    copies[-1].start()
    for copy in copies:
        copy.wait()


def body(across, along, populations, pore):
    count, planes, rows, columns = populations.shape
    height = across * rows
    width = columns // across
    tall = height + ROWS
    wide = width + LANES
    groups = -(-(count + 1) * planes * 4 // LANES)
    post, mask = pl.pallas_call(
        functools.partial(kernel, across, along),
        out_shape=(
            pltpu.VMEM((count, planes, tall, wide), jnp.float32),
            pltpu.VMEM((planes, tall, wide), jnp.float32),
        ),
        in_specs=[pl.BlockSpec(memory_space=pltpu.HBM)] * 2,
        out_specs=[pl.BlockSpec(memory_space=pltpu.VMEM)] * 2,
        scratch_shapes=[
            pltpu.VMEM((count + 1, planes, tall, wide), jnp.float32),
            pltpu.VMEM((count + 1, planes, rows, columns), jnp.float32),
            pltpu.VMEM((planes, rows, columns), jnp.int32),
            pltpu.VMEM((across, groups, rows, LANES), jnp.float32),
            pltpu.VMEM((groups, tall, LANES), jnp.float32),
            pltpu.SemaphoreType.DMA((3,)),
            pltpu.SemaphoreType.DMA((across,)),
            pltpu.SemaphoreType.DMA((across,)),
            pltpu.SemaphoreType.DMA((across,)),
            pltpu.SemaphoreType.DMA((across,)),
            pltpu.SemaphoreType.DMA((across,)),
            pltpu.SemaphoreType.DMA((across,)),
            pltpu.SemaphoreType.DMA((4,)),
            pltpu.SemaphoreType.DMA((4,)),
        ],
        compiler_params=pltpu.CompilerParams(
            collective_id=0, has_side_effects=True, vmem_limit_bytes=VMEM_LIMIT
        ),
    )(*(pltpu.with_memory_space_constraint(x, pltpu.HBM) for x in (populations, pore)))
    return pl.pallas_call(
        finish,
        out_shape=jax.ShapeDtypeStruct((count, planes, height, width), jnp.float32),
        in_specs=[pl.BlockSpec(memory_space=pltpu.VMEM)] * 2,
        out_specs=pl.BlockSpec(memory_space=pl.ANY),
        scratch_shapes=[
            pltpu.VMEM((count, planes, height, width), jnp.float32),
            pltpu.SemaphoreType.DMA((count,)),
        ],
        compiler_params=pltpu.CompilerParams(vmem_limit_bytes=VMEM_LIMIT),
    )(post, mask)


def solution(mesh):
    return jax.shard_map(
        functools.partial(body, mesh.shape["px"], mesh.shape["py"]),
        mesh=mesh,
        in_specs=(P(None, None, ("py", "px"), None), P(None, ("py", "px"), None)),
        out_specs=P(None, None, "py", "px"),
        check_vma=False,
    )
```

```python
import functools

import jax
import jax.numpy as jnp
from jax import lax
from jax.experimental import pallas as pl
from jax.experimental.pallas import tpu as pltpu
from jax.sharding import PartitionSpec as P

STEPS = 2
MESH = pl.DeviceIdType.MESH

lattice_velocity = [
    (0, 0, 0),
    (1, 0, 0),
    (-1, 0, 0),
    (0, 1, 0),
    (0, -1, 0),
    (0, 0, 1),
    (0, 0, -1),
    (1, 1, 0),
    (-1, -1, 0),
    (1, -1, 0),
    (-1, 1, 0),
    (1, 0, 1),
    (-1, 0, -1),
    (1, 0, -1),
    (-1, 0, 1),
    (0, 1, 1),
    (0, -1, -1),
    (0, 1, -1),
    (0, -1, 1),
]
lattice_weights = [1.0 / 3.0] + [1.0 / 18.0] * 6 + [1.0 / 36.0] * 12
opposite = [0, 2, 1, 4, 3, 6, 5, 8, 7, 10, 9, 12, 11, 14, 13, 16, 15, 18, 17]
relax_time = 0.8
body_force = 0.005

Q = len(lattice_velocity)
LANES = 128
ROWS = 8
HALO = 2
VMEM_LIMIT = 24 * 1024 * 1024
SOLID = -3.0e38


def collide_tile(fields, fluid):
    keep = 1.0 - 1.0 / relax_time
    gain = 1.0 / relax_time
    is_open = fluid > 0.5
    density = functools.reduce(lambda x, y: x + y, fields)
    density = jnp.where(is_open, density, 1.0)
    inverse = 1.0 / density
    vel = []
    for column in range(3):
        plus = [fields[s] for s in range(Q) if lattice_velocity[s][column] > 0]
        minus = [fields[s] for s in range(Q) if lattice_velocity[s][column] < 0]
        total = functools.reduce(lambda x, y: x + y, plus) - functools.reduce(lambda x, y: x + y, minus)
        vel.append(total * inverse)
    vel[2] = vel[2] + relax_time * body_force
    speed = vel[0] * vel[0] + vel[1] * vel[1] + vel[2] * vel[2]
    base = 1.0 - 1.5 * speed
    result = [None] * Q
    scaled = {w: density * (gain * w) for w in sorted(set(lattice_weights))}
    result[0] = jnp.where(is_open, keep * fields[0] + scaled[lattice_weights[0]] * base, SOLID)
    for slot in range(1, Q, 2):
        other = opposite[slot]
        along = None
        for column in range(3):
            sign = lattice_velocity[slot][column]
            if sign == 0:
                continue
            term = vel[column]
            if along is None:
                along = term if sign > 0 else -term
            else:
                along = along + term if sign > 0 else along - term
        weight = scaled[lattice_weights[slot]]
        triple = 3.0 * along
        even = weight * (base + 0.5 * triple * triple)
        odd = weight * triple
        result[slot] = jnp.where(is_open, keep * fields[slot] + (even + odd), SOLID)
        result[other] = jnp.where(is_open, keep * fields[other] + (even - odd), SOLID)
    return result


def kernel(
    across, along, pop_ref, pore_ref, post, mask,
    cells, strip, voxels, packs, edges,
    local_sem, a_send, a_recv, b_send, b_recv, e_send, e_recv, h_send, h_recv,
):
    _, planes, rows, _ = pop_ref.shape
    height = across * rows
    width = pop_ref.shape[3] // across
    tall = height + ROWS
    wide = width + LANES
    groups = edges.shape[0]
    per_group = LANES // 4
    me = lax.axis_index("px")
    here = lax.axis_index("py")
    up = lax.rem(here + along - 1, along)
    down = lax.rem(here + 1, along)

    own_rows = pl.ds(pl.multiple_of(me * rows, rows), rows)
    own_cols = pl.ds(pl.multiple_of(me * width, width), width)
    load_pore = pltpu.make_async_copy(pore_ref, voxels, local_sem.at[0])
    load_own = pltpu.make_async_copy(
        pop_ref.at[:, :, :, own_cols], cells.at[0:Q, :, own_rows, 0:width], local_sem.at[1]
    )
    load_strip = []
    for step in range(1, across + 1):
        cols = pl.ds(pl.multiple_of(lax.rem(me + step, across) * width, width), width)
        load_strip.append(
            pltpu.make_async_copy(
                pop_ref.at[:, :, :, cols], strip.at[0:Q, :, :, cols], local_sem.at[1 + step]
            )
        )
    load_pore.start()
    for copy in load_strip:
        copy.start()
    load_own.start()

    barrier = pltpu.get_barrier_semaphore()
    for step in range(1, across):
        pl.semaphore_signal(barrier, inc=1, device_id=(lax.rem(me + step, across), here), device_id_type=MESH)
    for to in (up, down):
        pl.semaphore_signal(barrier, inc=1, device_id=(me, to), device_id_type=MESH)

    load_pore.wait()
    strip[Q] = voxels[...].astype(jnp.float32)
    for copy in load_strip[:-1]:
        copy.wait()
    pl.semaphore_wait(barrier, across - 1 + 2)

    def near(source):
        return (rows - HALO, rows) if source == across - 1 else (0, HALO)

    def far(source):
        return (0, rows - HALO) if source == across - 1 else (HALO, rows)

    def strip_copy(source, target, part, cols, send, recv):
        low, high = part(source)
        start = target * width
        return pltpu.make_async_remote_copy(
            src_ref=strip.at[:, :, low:high, start + cols[0] : start + cols[1]],
            dst_ref=cells.at[:, :, source * rows + low : source * rows + high, cols[0] : cols[1]],
            send_sem=send,
            recv_sem=recv,
            device_id=(target, here),
            device_id_type=MESH,
        )

    def near_copy(source, target):
        return strip_copy(source, target, near, (0, width), a_send.at[target], a_recv.at[source])

    pieces = [(col, col + LANES) for col in range(0, width, LANES)]

    def far_copies(source, target):
        return [
            strip_copy(source, target, far, cols, b_send.at[target, n], b_recv.at[source, n])
            for n, cols in enumerate(pieces)
        ]

    def edge_copy(source, target):
        return pltpu.make_async_remote_copy(
            src_ref=packs.at[target],
            dst_ref=edges.at[:, source * rows : (source + 1) * rows, :],
            send_sem=e_send.at[target],
            recv_sem=e_recv.at[source],
            device_id=(target, here),
            device_id_type=MESH,
        )

    def halo_copies(way):
        if way == 0:
            source, dest, to = 0, height, up
        else:
            source, dest, to = height - HALO, tall - HALO, down
        return [
            pltpu.make_async_remote_copy(
                src_ref=cells.at[:, :, source : source + HALO, 0:width],
                dst_ref=cells.at[:, :, dest : dest + HALO, 0:width],
                send_sem=h_send.at[2 * way],
                recv_sem=h_recv.at[2 * way],
                device_id=(me, to),
                device_id_type=MESH,
            ),
            pltpu.make_async_remote_copy(
                src_ref=edges.at[:, source : source + HALO, :],
                dst_ref=edges.at[:, dest : dest + HALO, :],
                send_sem=h_send.at[2 * way + 1],
                recv_sem=h_recv.at[2 * way + 1],
                device_id=(me, to),
                device_id_type=MESH,
            ),
        ]

    def peers(mine):
        return [(mine + step) % across for step in range(1, across)]

    def on_each(action):
        for mine in range(across):
            pl.when(me == mine)(functools.partial(action, mine))

    def send_near(mine):
        for target in peers(mine):
            near_copy(mine, target).start()

    on_each(send_near)
    load_strip[-1].wait()

    lane = lax.broadcasted_iota(jnp.int32, (rows, LANES), 1)
    total = across * width
    for target in range(across):
        first = (target + 1) * width % total
        last = (target * width - LANES) % total
        for group in range(groups):
            packed = jnp.zeros((rows, LANES), jnp.float32)
            for place in range(per_group):
                slab = group * per_group + place
                if slab >= (Q + 1) * planes:
                    break
                field, plane = slab // planes, slab % planes
                edge = jnp.where(
                    lane < LANES // 2,
                    strip[field, plane, :, first : first + LANES],
                    strip[field, plane, :, last : last + LANES],
                )
                if place == 0:
                    packed = edge
                else:
                    moved = pltpu.roll(edge, 4 * place, 1)
                    packed = jnp.where((lane >= 4 * place - 2) & (lane < 4 * place + 2), moved, packed)
            packs[target, group] = packed

    ends = ((0, 0), (across - 1, 1))

    def send_rest(mine):
        for target in peers(mine):
            edge_copy(mine, target).start()
        for target in peers(mine):
            for copy in far_copies(mine, target):
                copy.start()

    on_each(send_rest)
    edges[:, own_rows, :] = packs[me]
    cells[Q, :, own_rows, 0:width] = voxels[:, :, own_cols].astype(jnp.float32)
    load_own.wait()

    def unpack(tile):
        at = pl.ds(pl.multiple_of(tile * ROWS, ROWS), ROWS)
        for slab in range((Q + 1) * planes):
            group, place = slab // per_group, slab % per_group
            packed = edges[group, at, :]
            moved = pltpu.roll(packed, LANES - 4 * place, 1) if place else packed
            cells[slab // planes, slab % planes, at, width:wide] = moved

    def collide(tile, columns):
        at = pl.ds(pl.multiple_of(tile * ROWS, ROWS), ROWS)
        for plane in range(planes):
            for col in columns:
                fields = [cells[slot, plane, at, col : col + LANES] for slot in range(Q)]
                result = collide_tile(fields, cells[Q, plane, at, col : col + LANES])
                for slot in range(Q):
                    post[slot, plane, at, col : col + LANES] = result[slot]

    tiles = tall // ROWS
    per_strip = rows // ROWS
    all_columns = range(0, wide, LANES)

    def relay_own(mine):
        for source, way in ends:
            if source == mine:
                for copy in halo_copies(way):
                    copy.start()

    on_each(relay_own)
    for part in range(per_strip):
        unpack(me * per_strip + part)
        collide(me * per_strip + part, all_columns)

    def relay(mine):
        for source, way in ends:
            if source != mine:
                near_copy(source, mine).wait_recv()
                edge_copy(source, mine).wait_recv()
                for copy in halo_copies(way):
                    copy.start()
        for source in peers(mine):
            if source not in (0, across - 1):
                near_copy(source, mine).wait_recv()
                edge_copy(source, mine).wait_recv()

    on_each(relay)

    def source_at(step):
        return lax.rem(me + step, across)

    def take_piece(step, n):
        source = source_at(step)
        low, high = pieces[n]
        arrived = cells.at[:, :, 0 : rows - HALO, low:high]
        pltpu.make_async_copy(arrived, arrived, b_recv.at[source, n]).wait()
        for part in range(per_strip):
            collide(source * per_strip + part, (low,))

    def take_edges(step, carry):
        for part in range(per_strip):
            unpack(source_at(step) * per_strip + part)
            collide(source_at(step) * per_strip + part, (width,))
        return carry

    def take_most(step, carry):
        for n in range(len(pieces) - 1):
            take_piece(step, n)
        return carry

    def take_last(step, carry):
        take_piece(step, len(pieces) - 1)
        return carry

    lax.fori_loop(1, across, take_edges, 0)
    lax.fori_loop(1, across, take_most, 0)
    for way in range(2):
        for copy in halo_copies(way):
            copy.wait_recv()
    unpack(tiles - 1)
    collide(tiles - 1, all_columns)
    lax.fori_loop(1, across, take_last, 0)

    def sent(mine):
        for target in peers(mine):
            near_copy(mine, target).wait_send()
            edge_copy(mine, target).wait_send()
            for copy in far_copies(mine, target):
                copy.wait_send()
        for way in range(2):
            for copy in halo_copies(way):
                copy.wait_send()

    on_each(sent)

    def collide_all(tile, carry):
        collide(tile, all_columns)
        return carry

    for step in range(STEPS):
        if step:
            lax.fori_loop(0, tiles, collide_all, 0)
        if step < STEPS - 1:
            for plane in range(planes):
                is_open = cells[Q, plane] > 0.5
                for slot in range(Q):
                    cells[slot, plane] = streamed(post, is_open, slot, plane)
    mask[...] = cells[Q]


def streamed(post, is_open, slot, plane):
    _, planes, tall, wide = post.shape
    vector = lattice_velocity[slot]
    value = post[slot, (plane - vector[2]) % planes]
    if vector[1]:
        value = pltpu.roll(value, vector[1] % tall, 0)
    if vector[0]:
        value = pltpu.roll(value, vector[0] % wide, 1)
    if slot:
        value = jnp.where(value != SOLID, value, post[opposite[slot], plane])
    return jnp.where(is_open, value, 0.0)


def finish(post, mask, out_ref, flow, sems):
    _, planes, height, width = flow.shape
    copies = []
    for slot in range(Q):
        for plane in range(planes):
            value = streamed(post, mask[plane] > 0.5, slot, plane)
            flow[slot, plane] = value[:height, :width]
        copies.append(pltpu.make_async_copy(flow.at[slot], out_ref.at[slot], sems.at[slot]))
        if slot:
            copies[slot - 1].start()
    copies[-1].start()
    for copy in copies:
        copy.wait()


def body(across, along, populations, pore):
    count, planes, rows, columns = populations.shape
    height = across * rows
    width = columns // across
    tall = height + ROWS
    wide = width + LANES
    groups = -(-(count + 1) * planes * 4 // LANES)
    post, mask = pl.pallas_call(
        functools.partial(kernel, across, along),
        out_shape=(
            pltpu.VMEM((count, planes, tall, wide), jnp.float32),
            pltpu.VMEM((planes, tall, wide), jnp.float32),
        ),
        in_specs=[pl.BlockSpec(memory_space=pltpu.HBM)] * 2,
        out_specs=[pl.BlockSpec(memory_space=pltpu.VMEM)] * 2,
        scratch_shapes=[
            pltpu.VMEM((count + 1, planes, tall, wide), jnp.float32),
            pltpu.VMEM((count + 1, planes, rows, columns), jnp.float32),
            pltpu.VMEM((planes, rows, columns), jnp.int32),
            pltpu.VMEM((across, groups, rows, LANES), jnp.float32),
            pltpu.VMEM((groups, tall, LANES), jnp.float32),
            pltpu.SemaphoreType.DMA((2 + across,)),
            pltpu.SemaphoreType.DMA((across,)),
            pltpu.SemaphoreType.DMA((across,)),
            pltpu.SemaphoreType.DMA((across, width // LANES)),
            pltpu.SemaphoreType.DMA((across, width // LANES)),
            pltpu.SemaphoreType.DMA((across,)),
            pltpu.SemaphoreType.DMA((across,)),
            pltpu.SemaphoreType.DMA((4,)),
            pltpu.SemaphoreType.DMA((4,)),
        ],
        compiler_params=pltpu.CompilerParams(
            collective_id=0, has_side_effects=True, vmem_limit_bytes=VMEM_LIMIT
        ),
    )(*(pltpu.with_memory_space_constraint(x, pltpu.HBM) for x in (populations, pore)))
    return pl.pallas_call(
        finish,
        out_shape=jax.ShapeDtypeStruct((count, planes, height, width), jnp.float32),
        in_specs=[pl.BlockSpec(memory_space=pltpu.VMEM)] * 2,
        out_specs=pl.BlockSpec(memory_space=pl.ANY),
        scratch_shapes=[
            pltpu.VMEM((count, planes, height, width), jnp.float32),
            pltpu.SemaphoreType.DMA((count,)),
        ],
        compiler_params=pltpu.CompilerParams(vmem_limit_bytes=VMEM_LIMIT),
    )(post, mask)


def solution(mesh):
    return jax.shard_map(
        functools.partial(body, mesh.shape["px"], mesh.shape["py"]),
        mesh=mesh,
        in_specs=(P(None, None, ("py", "px"), None), P(None, ("py", "px"), None)),
        out_specs=P(None, None, "py", "px"),
        check_vma=False,
    )
```

```python
import functools

import jax
import jax.numpy as jnp
from jax import lax
from jax.experimental import pallas as pl
from jax.experimental.pallas import tpu as pltpu
from jax.sharding import PartitionSpec as P

STEPS = 2
MESH = pl.DeviceIdType.MESH

lattice_velocity = [
    (0, 0, 0),
    (1, 0, 0),
    (-1, 0, 0),
    (0, 1, 0),
    (0, -1, 0),
    (0, 0, 1),
    (0, 0, -1),
    (1, 1, 0),
    (-1, -1, 0),
    (1, -1, 0),
    (-1, 1, 0),
    (1, 0, 1),
    (-1, 0, -1),
    (1, 0, -1),
    (-1, 0, 1),
    (0, 1, 1),
    (0, -1, -1),
    (0, 1, -1),
    (0, -1, 1),
]
lattice_weights = [1.0 / 3.0] + [1.0 / 18.0] * 6 + [1.0 / 36.0] * 12
opposite = [0, 2, 1, 4, 3, 6, 5, 8, 7, 10, 9, 12, 11, 14, 13, 16, 15, 18, 17]
relax_time = 0.8
body_force = 0.005

Q = len(lattice_velocity)
LANES = 128
ROWS = 8
HALO = 2
VMEM_LIMIT = 24 * 1024 * 1024
SOLID = -3.0e38


def collide_tile(fields, fluid):
    keep = 1.0 - 1.0 / relax_time
    gain = 1.0 / relax_time
    is_open = fluid > 0.5
    density = functools.reduce(lambda x, y: x + y, fields)
    density = jnp.where(is_open, density, 1.0)
    inverse = 1.0 / density
    vel = []
    for column in range(3):
        plus = [fields[s] for s in range(Q) if lattice_velocity[s][column] > 0]
        minus = [fields[s] for s in range(Q) if lattice_velocity[s][column] < 0]
        total = functools.reduce(lambda x, y: x + y, plus) - functools.reduce(lambda x, y: x + y, minus)
        vel.append(total * inverse)
    vel[2] = vel[2] + relax_time * body_force
    speed = vel[0] * vel[0] + vel[1] * vel[1] + vel[2] * vel[2]
    base = 1.0 - 1.5 * speed
    result = [None] * Q
    scaled = {w: density * (gain * w) for w in sorted(set(lattice_weights))}
    result[0] = jnp.where(is_open, keep * fields[0] + scaled[lattice_weights[0]] * base, SOLID)
    for slot in range(1, Q, 2):
        other = opposite[slot]
        along = None
        for column in range(3):
            sign = lattice_velocity[slot][column]
            if sign == 0:
                continue
            term = vel[column]
            if along is None:
                along = term if sign > 0 else -term
            else:
                along = along + term if sign > 0 else along - term
        weight = scaled[lattice_weights[slot]]
        triple = 3.0 * along
        even = weight * (base + 0.5 * triple * triple)
        odd = weight * triple
        result[slot] = jnp.where(is_open, keep * fields[slot] + (even + odd), SOLID)
        result[other] = jnp.where(is_open, keep * fields[other] + (even - odd), SOLID)
    return result


def kernel(
    across, along, pop_ref, pore_ref, post, mask,
    cells, strip, voxels, packs, edges,
    local_sem, a_send, a_recv, b_send, b_recv, e_send, e_recv, h_send, h_recv, w_send,
):
    _, planes, rows, _ = pop_ref.shape
    height = across * rows
    width = pop_ref.shape[3] // across
    tall = height + ROWS
    wide = width + LANES
    groups = edges.shape[0]
    per_group = LANES // 4
    me = lax.axis_index("px")
    here = lax.axis_index("py")
    up = lax.rem(here + along - 1, along)
    down = lax.rem(here + 1, along)

    own_rows = pl.ds(pl.multiple_of(me * rows, rows), rows)
    own_cols = pl.ds(pl.multiple_of(me * width, width), width)
    load_pore = pltpu.make_async_copy(pore_ref, voxels, local_sem.at[0])
    load_own = pltpu.make_async_copy(
        pop_ref.at[:, :, :, own_cols], cells.at[0:Q, :, own_rows, 0:width], local_sem.at[1]
    )
    load_strip = []
    for step in range(1, across + 1):
        cols = pl.ds(pl.multiple_of(lax.rem(me + step, across) * width, width), width)
        load_strip.append(
            pltpu.make_async_copy(
                pop_ref.at[:, :, :, cols], strip.at[0:Q, :, :, cols], local_sem.at[1 + step]
            )
        )
    load_pore.start()
    for copy in load_strip:
        copy.start()
    load_own.start()

    barrier = pltpu.get_barrier_semaphore()
    for step in range(1, across):
        pl.semaphore_signal(barrier, inc=1, device_id=(lax.rem(me + step, across), here), device_id_type=MESH)
    for to in (up, down):
        pl.semaphore_signal(barrier, inc=1, device_id=(me, to), device_id_type=MESH)

    corner = jnp.logical_and(me == across - 1, here == along - 1)

    @pl.when(jnp.logical_and(me != across - 1, here == 0))
    def _():
        pl.semaphore_signal(barrier, inc=1, device_id=(across - 1, along - 1), device_id_type=MESH)

    load_pore.wait()
    strip[Q] = voxels[...].astype(jnp.float32)
    for copy in load_strip[:-1]:
        copy.wait()
    greeted = across - 1 + 2

    @pl.when(corner)
    def _():
        pl.semaphore_wait(barrier, greeted + across - 1)

    @pl.when(jnp.logical_not(corner))
    def _():
        pl.semaphore_wait(barrier, greeted)

    def near(source):
        return (rows - HALO, rows) if source == across - 1 else (0, HALO)

    def far(source):
        return (0, rows - HALO) if source == across - 1 else (HALO, rows)

    def strip_copy(source, target, part, cols, send, recv):
        low, high = part(source)
        start = target * width
        return pltpu.make_async_remote_copy(
            src_ref=strip.at[:, :, low:high, start + cols[0] : start + cols[1]],
            dst_ref=cells.at[:, :, source * rows + low : source * rows + high, cols[0] : cols[1]],
            send_sem=send,
            recv_sem=recv,
            device_id=(target, here),
            device_id_type=MESH,
        )

    def near_copy(source, target):
        return strip_copy(source, target, near, (0, width), a_send.at[target], a_recv.at[source])

    pieces = [(col, col + LANES) for col in range(0, width, LANES)]

    def far_copies(source, target):
        return [
            strip_copy(source, target, far, cols, b_send.at[target, n], b_recv.at[source, n])
            for n, cols in enumerate(pieces)
        ]

    def edge_copy(source, target):
        return pltpu.make_async_remote_copy(
            src_ref=packs.at[target],
            dst_ref=edges.at[:, source * rows : (source + 1) * rows, :],
            send_sem=e_send.at[target],
            recv_sem=e_recv.at[source],
            device_id=(target, here),
            device_id_type=MESH,
        )

    def halo_copies(way):
        if way == 0:
            source, dest, to = 0, height, up
        else:
            source, dest, to = height - HALO, tall - HALO, down
        return [
            pltpu.make_async_remote_copy(
                src_ref=cells.at[:, :, source : source + HALO, 0:width],
                dst_ref=cells.at[:, :, dest : dest + HALO, 0:width],
                send_sem=h_send.at[2 * way],
                recv_sem=h_recv.at[2 * way],
                device_id=(me, to),
                device_id_type=MESH,
            ),
            pltpu.make_async_remote_copy(
                src_ref=edges.at[:, source : source + HALO, :],
                dst_ref=edges.at[:, dest : dest + HALO, :],
                send_sem=h_send.at[2 * way + 1],
                recv_sem=h_recv.at[2 * way + 1],
                device_id=(me, to),
                device_id_type=MESH,
            ),
        ]

    def wrap_rows(target):
        return pltpu.make_async_remote_copy(
            src_ref=strip.at[:, :, rows - HALO : rows, target * width : (target + 1) * width],
            dst_ref=cells.at[:, :, tall - HALO : tall, 0:width],
            send_sem=w_send.at[0, target],
            recv_sem=h_recv.at[2],
            device_id=(target, 0),
            device_id_type=MESH,
        )

    def wrap_edges(target):
        return pltpu.make_async_remote_copy(
            src_ref=packs.at[target, :, rows - HALO : rows, :],
            dst_ref=edges.at[:, tall - HALO : tall, :],
            send_sem=w_send.at[1, target],
            recv_sem=h_recv.at[3],
            device_id=(target, 0),
            device_id_type=MESH,
        )

    def peers(mine):
        return [(mine + step) % across for step in range(1, across)]

    def on_each(action):
        for mine in range(across):
            pl.when(me == mine)(functools.partial(action, mine))

    def send_near(mine):
        for target in peers(mine):
            near_copy(mine, target).start()

    @pl.when(corner)
    def _():
        for target in range(across - 1):
            wrap_rows(target).start()

    on_each(send_near)
    load_strip[-1].wait()

    lane = lax.broadcasted_iota(jnp.int32, (rows, LANES), 1)
    total = across * width
    for target in range(across):
        first = (target + 1) * width % total
        last = (target * width - LANES) % total
        for group in range(groups):
            packed = jnp.zeros((rows, LANES), jnp.float32)
            for place in range(per_group):
                slab = group * per_group + place
                if slab >= (Q + 1) * planes:
                    break
                field, plane = slab // planes, slab % planes
                edge = jnp.where(
                    lane < LANES // 2,
                    strip[field, plane, :, first : first + LANES],
                    strip[field, plane, :, last : last + LANES],
                )
                if place == 0:
                    packed = edge
                else:
                    moved = pltpu.roll(edge, 4 * place, 1)
                    packed = jnp.where((lane >= 4 * place - 2) & (lane < 4 * place + 2), moved, packed)
            packs[target, group] = packed

    ends = ((0, 0), (across - 1, 1))

    def send_rest(mine):
        for target in peers(mine):
            edge_copy(mine, target).start()
        for target in peers(mine):
            for copy in far_copies(mine, target):
                copy.start()

    @pl.when(corner)
    def _():
        for target in range(across - 1):
            wrap_edges(target).start()

    on_each(send_rest)
    edges[:, own_rows, :] = packs[me]
    cells[Q, :, own_rows, 0:width] = voxels[:, :, own_cols].astype(jnp.float32)
    load_own.wait()

    def unpack(tile):
        at = pl.ds(pl.multiple_of(tile * ROWS, ROWS), ROWS)
        for slab in range((Q + 1) * planes):
            group, place = slab // per_group, slab % per_group
            packed = edges[group, at, :]
            moved = pltpu.roll(packed, LANES - 4 * place, 1) if place else packed
            cells[slab // planes, slab % planes, at, width:wide] = moved

    def collide(tile, columns):
        at = pl.ds(pl.multiple_of(tile * ROWS, ROWS), ROWS)
        for plane in range(planes):
            for col in columns:
                fields = [cells[slot, plane, at, col : col + LANES] for slot in range(Q)]
                result = collide_tile(fields, cells[Q, plane, at, col : col + LANES])
                for slot in range(Q):
                    post[slot, plane, at, col : col + LANES] = result[slot]

    tiles = tall // ROWS
    per_strip = rows // ROWS
    all_columns = range(0, wide, LANES)

    def relay_own(mine):
        for source, way in ends:
            if source == mine:
                for copy in halo_copies(way):
                    copy.start()

    on_each(relay_own)
    for part in range(per_strip):
        unpack(me * per_strip + part)
        collide(me * per_strip + part, all_columns)

    def relay(mine):
        for source, way in ends:
            if source != mine:
                near_copy(source, mine).wait_recv()
                edge_copy(source, mine).wait_recv()

                @pl.when(jnp.logical_or(way == 0, here != along - 1))
                def _():
                    for copy in halo_copies(way):
                        copy.start()

        for source in peers(mine):
            if source not in (0, across - 1):
                near_copy(source, mine).wait_recv()
                edge_copy(source, mine).wait_recv()

    on_each(relay)

    def source_at(step):
        return lax.rem(me + step, across)

    def take_piece(step, n):
        source = source_at(step)
        low, high = pieces[n]
        arrived = cells.at[:, :, 0 : rows - HALO, low:high]
        pltpu.make_async_copy(arrived, arrived, b_recv.at[source, n]).wait()
        for part in range(per_strip):
            collide(source * per_strip + part, (low,))

    def take_edges(step, carry):
        for part in range(per_strip):
            unpack(source_at(step) * per_strip + part)
            collide(source_at(step) * per_strip + part, (width,))
        return carry

    def take_most(step, carry):
        for n in range(len(pieces) - 1):
            take_piece(step, n)
        return carry

    def take_last(step, carry):
        take_piece(step, len(pieces) - 1)
        return carry

    lax.fori_loop(1, across, take_edges, 0)
    lax.fori_loop(1, across, take_most, 0)
    for way in range(2):
        for copy in halo_copies(way):
            copy.wait_recv()
    unpack(tiles - 1)
    collide(tiles - 1, all_columns)
    lax.fori_loop(1, across, take_last, 0)

    def sent(mine):
        for target in peers(mine):
            near_copy(mine, target).wait_send()
            edge_copy(mine, target).wait_send()
            for copy in far_copies(mine, target):
                copy.wait_send()
        for source, way in ends:

            @pl.when(jnp.logical_or(way == 0 or source == mine, here != along - 1))
            def _():
                for copy in halo_copies(way):
                    copy.wait_send()

    on_each(sent)

    @pl.when(corner)
    def _():
        for target in range(across - 1):
            wrap_rows(target).wait_send()
            wrap_edges(target).wait_send()

    def collide_all(tile, carry):
        collide(tile, all_columns)
        return carry

    for step in range(STEPS):
        if step:
            lax.fori_loop(0, tiles, collide_all, 0)
        if step < STEPS - 1:
            for plane in range(planes):
                is_open = cells[Q, plane] > 0.5
                for slot in range(Q):
                    cells[slot, plane] = streamed(post, is_open, slot, plane)
    mask[...] = cells[Q]


def streamed(post, is_open, slot, plane):
    _, planes, tall, wide = post.shape
    vector = lattice_velocity[slot]
    value = post[slot, (plane - vector[2]) % planes]
    if vector[1]:
        value = pltpu.roll(value, vector[1] % tall, 0)
    if vector[0]:
        value = pltpu.roll(value, vector[0] % wide, 1)
    if slot:
        value = jnp.where(value != SOLID, value, post[opposite[slot], plane])
    return jnp.where(is_open, value, 0.0)


def finish(post, mask, out_ref, flow, sems):
    _, planes, height, width = flow.shape
    copies = []
    for slot in range(Q):
        for plane in range(planes):
            value = streamed(post, mask[plane] > 0.5, slot, plane)
            flow[slot, plane] = value[:height, :width]
        copies.append(pltpu.make_async_copy(flow.at[slot], out_ref.at[slot], sems.at[slot]))
        if slot:
            copies[slot - 1].start()
    copies[-1].start()
    for copy in copies:
        copy.wait()


def body(across, along, populations, pore):
    count, planes, rows, columns = populations.shape
    height = across * rows
    width = columns // across
    tall = height + ROWS
    wide = width + LANES
    groups = -(-(count + 1) * planes * 4 // LANES)
    post, mask = pl.pallas_call(
        functools.partial(kernel, across, along),
        out_shape=(
            pltpu.VMEM((count, planes, tall, wide), jnp.float32),
            pltpu.VMEM((planes, tall, wide), jnp.float32),
        ),
        in_specs=[pl.BlockSpec(memory_space=pltpu.HBM)] * 2,
        out_specs=[pl.BlockSpec(memory_space=pltpu.VMEM)] * 2,
        scratch_shapes=[
            pltpu.VMEM((count + 1, planes, tall, wide), jnp.float32),
            pltpu.VMEM((count + 1, planes, rows, columns), jnp.float32),
            pltpu.VMEM((planes, rows, columns), jnp.int32),
            pltpu.VMEM((across, groups, rows, LANES), jnp.float32),
            pltpu.VMEM((groups, tall, LANES), jnp.float32),
            pltpu.SemaphoreType.DMA((2 + across,)),
            pltpu.SemaphoreType.DMA((across,)),
            pltpu.SemaphoreType.DMA((across,)),
            pltpu.SemaphoreType.DMA((across, width // LANES)),
            pltpu.SemaphoreType.DMA((across, width // LANES)),
            pltpu.SemaphoreType.DMA((across,)),
            pltpu.SemaphoreType.DMA((across,)),
            pltpu.SemaphoreType.DMA((4,)),
            pltpu.SemaphoreType.DMA((4,)),
            pltpu.SemaphoreType.DMA((2, across)),
        ],
        compiler_params=pltpu.CompilerParams(
            collective_id=0, has_side_effects=True, vmem_limit_bytes=VMEM_LIMIT
        ),
    )(*(pltpu.with_memory_space_constraint(x, pltpu.HBM) for x in (populations, pore)))
    return pl.pallas_call(
        finish,
        out_shape=jax.ShapeDtypeStruct((count, planes, height, width), jnp.float32),
        in_specs=[pl.BlockSpec(memory_space=pltpu.VMEM)] * 2,
        out_specs=pl.BlockSpec(memory_space=pl.ANY),
        scratch_shapes=[
            pltpu.VMEM((count, planes, height, width), jnp.float32),
            pltpu.SemaphoreType.DMA((count,)),
        ],
        compiler_params=pltpu.CompilerParams(vmem_limit_bytes=VMEM_LIMIT),
    )(post, mask)


def solution(mesh):
    return jax.shard_map(
        functools.partial(body, mesh.shape["px"], mesh.shape["py"]),
        mesh=mesh,
        in_specs=(P(None, None, ("py", "px"), None), P(None, ("py", "px"), None)),
        out_specs=P(None, None, "py", "px"),
        check_vma=False,
    )
```
